8 devices in a mesh: col: 4 (over z, y, x), row: 2 (over core).
Axes of the slice: x: 2, y: 2, z: 1, core: 2. Of those that a mesh axis runs over, the one named last changes fastest.
Arguments:
- mask: int32 [4096, 65536], P('row', 'col')
- user_emb: bfloat16 [4096, 256], P(('row', 'col'))
- item_emb: bfloat16 [65536, 256], P(('col', 'row'))
- queries: int32 [512], replicated
Outputs:
- output 1: bfloat16 [4096, 256], P(('row', 'col'))
- output 2: bfloat16 [65536, 256], P(('col', 'row'))
- output 3: float32 [512, 65536], P(None, ('col', 'row'))
All inputs are finite; a program needn't handle non-finite values.
Results may differ from the reference program's by a relative error of at most 0.00683025.
Values are sent between devices in bfloat16 or wider.
A program may use at most 1 GiB of HBM per device.

```python
import jax
import jax.numpy as jnp
from jax import lax

USERS = 4096
ITEMS = 65536
EMB = 256
LAYERS = 3
QUERIES = 512


def draw_mask(key):
    k_noise, k_rows, k_cols = jax.random.split(key, 3)
    row_level = jax.random.randint(k_rows, (USERS,), 4, 33)
    col_level = jax.random.randint(k_cols, (ITEMS,), 4, 33)
    noise = jax.random.randint(k_noise, (USERS, ITEMS), 0, 1024)
    return (noise < row_level[:, None] * col_level[None, :]).astype(jnp.int32)


def setup_inputs(seed: int = 0) -> dict:
    key = jax.random.key(seed)
    k_mask, k_user, k_item, k_umean, k_imean, k_query = jax.random.split(key, 6)
    scale = EMB ** -0.25
    user_mean = jax.random.normal(k_umean, (EMB,), jnp.float32)
    item_mean = jax.random.normal(k_imean, (EMB,), jnp.float32)
    user_emb = ((jax.random.normal(k_user, (USERS, EMB), jnp.float32) + user_mean[None, :]) * scale).astype(jnp.bfloat16)
    item_emb = ((jax.random.normal(k_item, (ITEMS, EMB), jnp.float32) + item_mean[None, :]) * scale).astype(jnp.bfloat16)
    queries = jax.random.randint(k_query, (QUERIES,), 0, USERS).astype(jnp.int32)
    return {'mask': draw_mask(k_mask), 'user_emb': user_emb, 'item_emb': item_emb, 'queries': queries}


def norm_adjacency(mask):
    deg_user = jnp.maximum(jnp.sum(mask, axis=1), 1)
    deg_item = jnp.maximum(jnp.sum(mask, axis=0), 1)
    inv_user = lax.rsqrt(deg_user.astype(jnp.float32))
    inv_item = lax.rsqrt(deg_item.astype(jnp.float32))
    return (inv_user[:, None] * mask.astype(jnp.float32) * inv_item[None, :]).astype(jnp.bfloat16)


def reference(mask, user_emb, item_emb, queries):
    norm_adj = norm_adjacency(mask)

    def one_layer(carried, unused):
        user_cur, item_cur, user_sum, item_sum = carried
        user_next = jnp.dot(norm_adj, item_cur, preferred_element_type=jnp.float32).astype(jnp.bfloat16)
        item_next = lax.dot_general(norm_adj, user_cur, (((0,), (0,)), ((), ())), preferred_element_type=jnp.float32).astype(jnp.bfloat16)
        return (user_next, item_next, user_sum + user_next.astype(jnp.float32), item_sum + item_next.astype(jnp.float32)), None

    start_state = (user_emb, item_emb, user_emb.astype(jnp.float32), item_emb.astype(jnp.float32))
    end_state, unused_out = lax.scan(one_layer, start_state, None, length=LAYERS)
    final_user = (end_state[2] / (LAYERS + 1)).astype(jnp.bfloat16)
    final_item = (end_state[3] / (LAYERS + 1)).astype(jnp.bfloat16)
    picked = jnp.take(final_user, queries, axis=0)
    scores = lax.dot_general(picked, final_item, (((1,), (1,)), ((), ())), preferred_element_type=jnp.float32)
    return final_user, final_item, scores
```

```python
import functools

import jax
import jax.numpy as jnp
from jax import lax
from jax.experimental import pallas as pl
from jax.experimental.pallas import tpu as pltpu
from jax.sharding import PartitionSpec as P

LAYERS = 3
KT = 512
SLOTS = 10
SENDS = 4
VMEM_CAP = 60 * 1024 * 1024
MESH = pl.DeviceIdType.MESH
NN = (((1,), (0,)), ((), ()))
NT = (((1,), (1,)), ((), ()))


def pack_kernel(steps, mask_ref, bits_ref, rs_ref, cs_ref, row_acc):
    step = pl.program_id(0)
    rows, cols = mask_ref.shape

    @pl.when(step == 0)
    def _():
        row_acc[...] = jnp.zeros_like(row_acc)

    def block(b, col_acc):
        word = jnp.zeros((8, cols), jnp.int32)
        for j in range(32):
            at = pl.ds(pl.multiple_of(b * 256 + j * 8, 8), 8)
            m = mask_ref[at, :]
            word = word | lax.shift_left(m, j) if j else m
            col_acc = col_acc + m
            part = m[:, :128]
            for t in range(1, cols // 128):
                part = part + m[:, t * 128:(t + 1) * 128]
            row_acc[at, :] += part
        bits_ref[pl.ds(pl.multiple_of(b * 8, 8), 8), :] = word
        return col_acc

    col_acc = lax.fori_loop(0, rows // 256, block, jnp.zeros((8, cols), jnp.int32))
    cs_ref[...] = jnp.sum(col_acc, axis=0, keepdims=True)

    @pl.when(step == steps - 1)
    def _():
        for g in range(rows // 128):
            rs_ref[g:g + 1, :] = jnp.sum(row_acc[g * 128:(g + 1) * 128, :].T, axis=0, keepdims=True)


def pack(mask_blk):
    rows, cols = mask_blk.shape
    steps = cols // KT
    return pl.pallas_call(
        functools.partial(pack_kernel, steps),
        grid=(steps,),
        in_specs=[pl.BlockSpec((rows, KT), lambda i: (0, i))],
        out_specs=[pl.BlockSpec((rows // 32, KT), lambda i: (0, i)),
                   pl.BlockSpec((rows // 128, 128), lambda i: (0, 0)),
                   pl.BlockSpec((1, KT), lambda i: (0, i))],
        out_shape=[jax.ShapeDtypeStruct((rows // 32, cols), jnp.int32),
                   jax.ShapeDtypeStruct((rows // 128, 128), jnp.int32),
                   jax.ShapeDtypeStruct((1, cols), jnp.int32)],
        scratch_shapes=[pltpu.VMEM((rows, 128), jnp.int32)],
        compiler_params=pltpu.CompilerParams(dimension_semantics=('arbitrary',), vmem_limit_bytes=VMEM_CAP),
        name='pack',
    )(mask_blk)


def greet(peers):
    barrier = pltpu.get_barrier_semaphore()
    for dev in peers:
        pl.semaphore_signal(barrier, inc=1, device_id=dev, device_id_type=MESH)
    pl.semaphore_wait(barrier, len(peers))


def col_peer(col, row, n_col, off):
    return (lax.rem(col + off, n_col), row)


def degree_kernel(n_col, rs_ref, cs_ref, du_ref, di_ref, rs_in, cs_in, rs_send, rs_recv, cs_send, cs_recv):
    col, row = lax.axis_index('col'), lax.axis_index('row')
    other = (col, 1 - row)
    greet([other] + [col_peer(col, row, n_col, o) for o in range(1, n_col)])
    copies = [pltpu.make_async_remote_copy(src_ref=cs_ref, dst_ref=cs_in, send_sem=cs_send, recv_sem=cs_recv,
                                           device_id=other, device_id_type=MESH)]
    for o in range(1, n_col):
        copies.append(pltpu.make_async_remote_copy(
            src_ref=rs_ref, dst_ref=rs_in.at[o - 1], send_sem=rs_send.at[o - 1], recv_sem=rs_recv.at[o - 1],
            device_id=col_peer(col, row, n_col, o), device_id_type=MESH))
    for copy in copies:
        copy.start()
    for copy in copies:
        copy.wait()
    deg = rs_ref[...]
    for o in range(1, n_col):
        deg = deg + rs_in[o - 1]
    inv_user = lax.rsqrt(jnp.maximum(deg, 1).astype(jnp.float32))
    for g in range(inv_user.shape[0]):
        du_ref[g * 128:(g + 1) * 128, :] = jnp.broadcast_to(inv_user[g:g + 1, :], (128, 128)).T
    di_ref[...] = lax.rsqrt(jnp.maximum(cs_ref[...] + cs_in[...], 1).astype(jnp.float32))


def degrees(rs, cs, n_col):
    groups, cols = rs.shape[0], cs.shape[1]
    vmem = pl.BlockSpec(memory_space=pltpu.VMEM)
    return pl.pallas_call(
        functools.partial(degree_kernel, n_col),
        in_specs=[vmem, vmem],
        out_specs=[vmem, vmem],
        out_shape=[jax.ShapeDtypeStruct((groups * 128, 128), jnp.float32),
                   jax.ShapeDtypeStruct((1, cols), jnp.float32)],
        scratch_shapes=[pltpu.VMEM((n_col - 1,) + rs.shape, jnp.int32), pltpu.VMEM(cs.shape, jnp.int32),
                        pltpu.SemaphoreType.DMA((n_col - 1,)), pltpu.SemaphoreType.DMA((n_col - 1,)),
                        pltpu.SemaphoreType.DMA, pltpu.SemaphoreType.DMA],
        compiler_params=pltpu.CompilerParams(collective_id=0, has_side_effects=True),
        name='degrees',
    )(rs, cs)


def expand(bits_ref, du_ref, di, out_ref):
    cols = di.shape[1]

    def block(b, carry):
        word = bits_ref[pl.ds(pl.multiple_of(b * 8, 8), 8), :]
        for j in range(16):
            at = pl.multiple_of(b * 256 + j * 16, 16)
            halves = []
            for k in range(2):
                scale = du_ref[pl.ds(pl.multiple_of(at + k * 8, 8), 8), :]
                value = jnp.concatenate([scale] * (cols // 128), axis=1) * di
                hit = (word & (1 << (2 * j + k)) if 2 * j + k < 31 else word & (-2147483648)) != 0
                halves.append(jnp.where(hit, value, 0.0))
            out_ref[pl.ds(at, 16), :] = jnp.concatenate(halves, axis=0).astype(jnp.bfloat16)
        return carry

    lax.fori_loop(0, out_ref.shape[0] // 256, block, 0)


def adjacency_kernel(bits_ref, du_ref, di_ref, out_ref):
    expand(bits_ref, du_ref, jnp.broadcast_to(di_ref[...], (8, di_ref.shape[1])), out_ref.at[0])


def adjacency(bits, du, di):
    rows, cols = du.shape[0], bits.shape[1]
    steps = cols // KT
    return pl.pallas_call(
        adjacency_kernel,
        grid=(steps,),
        in_specs=[pl.BlockSpec((rows // 32, KT), lambda i: (0, i)),
                  pl.BlockSpec((rows, 128), lambda i: (0, 0)),
                  pl.BlockSpec((1, KT), lambda i: (0, i))],
        out_specs=pl.BlockSpec((1, rows, KT), lambda i: (i, 0, 0)),
        out_shape=jax.ShapeDtypeStruct((steps, rows, KT), jnp.bfloat16),
        compiler_params=pltpu.CompilerParams(dimension_semantics=('arbitrary',), vmem_limit_bytes=VMEM_CAP),
        name='adjacency',
    )(bits, du, di)


def layer_kernel(n_col, adj, item_own, user_own, item_next, user_next,
                 abuf, panel, acc, upan, ut, rs_in, ix_in, ix_out,
                 a_sem, own_sem, pan_send, pan_recv, uown_sem, u_send, u_recv, rs_send, rs_recv, ix_send, ix_recv):
    col, row = lax.axis_index('col'), lax.axis_index('row')
    other = (col, 1 - row)
    chunks = adj.shape[0]
    half = chunks // 2
    slots = abuf.shape[0]
    sends = ix_out.shape[0]
    own_rows = acc.shape[0] // n_col

    def user_chunk(t):
        return jnp.where(t < half, row * half + t, (1 - row) * half + t - half)

    def turn(q):
        return lax.rem(q + half - slots + half, half)

    def item_chunk(q):
        return jnp.where(q < half, (1 - row) * half + turn(q), row * half + turn(q - half))

    def load(chunk, slot):
        return pltpu.make_async_copy(adj.at[chunk], abuf.at[slot], a_sem.at[slot])

    greet([other] + [col_peer(col, row, n_col, o) for o in range(1, n_col)])

    own_copy = pltpu.make_async_copy(item_own, panel.at[0], own_sem)
    own_copy.start()
    pan_copy = pltpu.make_async_remote_copy(src_ref=item_own, dst_ref=panel.at[1], send_sem=pan_send,
                                            recv_sem=pan_recv, device_id=other, device_id_type=MESH)
    pan_copy.start()
    for t in range(slots - 1):
        load(user_chunk(t), t).start()
    uown_copy = pltpu.make_async_copy(user_own, upan.at[col], uown_sem)
    uown_copy.start()
    u_copies = [pltpu.make_async_remote_copy(
        src_ref=user_own, dst_ref=upan.at[col], send_sem=u_send.at[o - 1], recv_sem=u_recv.at[o - 1],
        device_id=col_peer(col, row, n_col, o), device_id_type=MESH) for o in range(1, n_col)]
    for copy in u_copies:
        copy.start()
    acc[...] = jnp.zeros_like(acc)
    own_copy.wait()

    def user_step(side, t, carry):
        slot = lax.rem(t, slots)

        @pl.when(t + slots - 1 < chunks)
        def _():
            load(user_chunk(t + slots - 1), lax.rem(t + slots - 1, slots)).start()

        load(user_chunk(t), slot).wait()
        at = pl.ds(pl.multiple_of((t - side * half) * KT, KT), KT)
        acc[...] += lax.dot_general(abuf[slot], panel[side, at, :], NN, preferred_element_type=jnp.float32)
        return carry

    lax.fori_loop(0, half, functools.partial(user_step, 0), 0)
    pan_copy.wait()
    lax.fori_loop(half, chunks, functools.partial(user_step, 1), 0)

    uown_copy.wait()
    for copy in u_copies:
        copy.wait()
    for c in range(n_col):
        ut[:, c * own_rows:(c + 1) * own_rows] = upan[c].T

    rs_copies = []
    for o in range(1, n_col):
        dest = lax.rem(col + o, n_col)
        rs_copies.append(pltpu.make_async_remote_copy(
            src_ref=acc.at[pl.ds(pl.multiple_of(dest * own_rows, own_rows), own_rows), :], dst_ref=rs_in.at[o - 1],
            send_sem=rs_send.at[o - 1], recv_sem=rs_recv.at[o - 1],
            device_id=(dest, row), device_id_type=MESH))
    for copy in rs_copies:
        copy.start()

    def ix_copy(q):
        return pltpu.make_async_remote_copy(
            src_ref=ix_out.at[lax.rem(q, sends)], dst_ref=ix_in.at[turn(q)], send_sem=ix_send.at[lax.rem(q, sends)],
            recv_sem=ix_recv.at[turn(q)], device_id=other, device_id_type=MESH)

    def product(q):
        slot = lax.rem(chunks + q, slots)

        @pl.when((q >= 1) & (q - 1 + slots < chunks))
        def _():
            load(item_chunk(q - 1 + slots), lax.rem(chunks + q - 1, slots)).start()

        @pl.when(q >= slots)
        def _():
            load(item_chunk(q), slot).wait()

        return lax.dot_general(ut[...], abuf[slot], NN, preferred_element_type=jnp.float32)

    def give_step(q, carry):
        part = product(q)

        @pl.when(q >= sends)
        def _():
            ix_copy(q - sends).wait_send()

        ix_out[lax.rem(q, sends)] = part
        ix_copy(q).start()
        return carry

    lax.fori_loop(0, half, give_step, 0)

    def keep_step(q, carry):
        part = product(q)
        j = turn(q - half)
        ix_copy(q - half).wait_recv()
        whole = (part + ix_in[j]).astype(jnp.bfloat16)
        item_next[pl.ds(pl.multiple_of(j * KT, KT), KT), :] = whole.T
        return carry

    lax.fori_loop(half, chunks, keep_step, 0)

    for q in range(half - sends, half):
        ix_copy(q).wait_send()
    for copy in rs_copies:
        copy.wait()
    total = acc[pl.ds(pl.multiple_of(col * own_rows, own_rows), own_rows), :]
    for o in range(1, n_col):
        total = total + rs_in[o - 1]
    user_next[...] = total.astype(jnp.bfloat16)


def layer(adj, item_own, user_own, n_col):
    chunks, rows, _ = adj.shape
    items, emb = item_own.shape
    users = user_own.shape[0]
    half = chunks // 2
    anyspace = pl.BlockSpec(memory_space=pl.ANY)
    vmem = pl.BlockSpec(memory_space=pltpu.VMEM)
    dma = pltpu.SemaphoreType.DMA
    flops = 4 * chunks * rows * KT * emb
    return pl.pallas_call(
        functools.partial(layer_kernel, n_col),
        in_specs=[anyspace, anyspace, anyspace],
        out_specs=[vmem, vmem],
        out_shape=[jax.ShapeDtypeStruct((items, emb), jnp.bfloat16),
                   jax.ShapeDtypeStruct((users, emb), jnp.bfloat16)],
        scratch_shapes=[
            pltpu.VMEM((SLOTS, rows, KT), jnp.bfloat16),
            pltpu.VMEM((2, items, emb), jnp.bfloat16),
            pltpu.VMEM((rows, emb), jnp.float32),
            pltpu.VMEM((n_col, users, emb), jnp.bfloat16),
            pltpu.VMEM((emb, rows), jnp.bfloat16),
            pltpu.VMEM((n_col - 1, users, emb), jnp.float32),
            pltpu.VMEM((half, emb, KT), jnp.float32),
            pltpu.VMEM((SENDS, emb, KT), jnp.float32),
            dma((SLOTS,)), dma, dma, dma, dma,
            dma((n_col - 1,)), dma((n_col - 1,)), dma((n_col - 1,)), dma((n_col - 1,)),
            dma((SENDS,)), dma((half,)),
        ],
        cost_estimate=pl.CostEstimate(flops=flops, bytes_accessed=adj.size * 4, transcendentals=0),
        compiler_params=pltpu.CompilerParams(collective_id=1, has_side_effects=True, vmem_limit_bytes=VMEM_CAP),
        name='layer',
    )(adj, item_own, user_own)


def pick_kernel(n_col, u0, u1, u2, u3, query, final_user, picked, mine, parts, one_send, one_recv, two_send, two_recv):
    col, row = lax.axis_index('col'), lax.axis_index('row')
    n_dev = 2 * n_col
    me = col * 2 + row
    share = picked.shape[0] // n_dev
    rows = u0.shape[0]

    def dev(o):
        lin = lax.rem(me + o, n_dev)
        return lin, (lin // 2, lin % 2)

    greet([dev(o)[1] for o in range(1, n_dev)])
    total = u0[...].astype(jnp.float32) + u1[...].astype(jnp.float32)
    total = total + u2[...].astype(jnp.float32)
    total = total + u3[...].astype(jnp.float32)
    final = (total / (LAYERS + 1)).astype(jnp.bfloat16)
    final_user[...] = final
    local = query[...] - (row * n_col + col) * rows
    hot = lax.broadcasted_iota(jnp.int32, (query.shape[0], rows), 1) == local
    mine[...] = jnp.dot(hot.astype(jnp.bfloat16), final, preferred_element_type=jnp.float32).astype(jnp.bfloat16)

    def rows_of(lin):
        return pl.ds(pl.multiple_of(lin * share, share), share)

    first = []
    for o in range(1, n_dev):
        lin, dest = dev(o)
        first.append(pltpu.make_async_remote_copy(
            src_ref=mine.at[rows_of(lin), :], dst_ref=parts.at[o - 1], send_sem=one_send.at[o - 1],
            recv_sem=one_recv.at[o - 1], device_id=dest, device_id_type=MESH))
    for copy in first:
        copy.start()
    for copy in first:
        copy.wait()
    found = mine[rows_of(me), :].astype(jnp.float32)
    for o in range(1, n_dev):
        found = found + parts[o - 1].astype(jnp.float32)
    picked[rows_of(me), :] = found.astype(jnp.bfloat16)
    second = []
    for o in range(1, n_dev):
        second.append(pltpu.make_async_remote_copy(
            src_ref=picked.at[rows_of(me), :], dst_ref=picked.at[rows_of(me), :], send_sem=two_send.at[o - 1],
            recv_sem=two_recv.at[o - 1], device_id=dev(o)[1], device_id_type=MESH))
    for copy in second:
        copy.start()
    for copy in second:
        copy.wait()


def pick(users, queries, n_col):
    n_dev = 2 * n_col
    rows, emb = users[0].shape
    n_query = queries.shape[0]
    vmem = pl.BlockSpec(memory_space=pltpu.VMEM)
    dma = pltpu.SemaphoreType.DMA
    return pl.pallas_call(
        functools.partial(pick_kernel, n_col),
        in_specs=[vmem] * 5,
        out_specs=[vmem, vmem],
        out_shape=[jax.ShapeDtypeStruct((rows, emb), jnp.bfloat16),
                   jax.ShapeDtypeStruct((n_query, emb), jnp.bfloat16)],
        scratch_shapes=[pltpu.VMEM((n_query, emb), jnp.bfloat16),
                        pltpu.VMEM((n_dev - 1, n_query // n_dev, emb), jnp.bfloat16),
                        dma((n_dev - 1,)), dma((n_dev - 1,)), dma((n_dev - 1,)), dma((n_dev - 1,))],
        compiler_params=pltpu.CompilerParams(collective_id=2, has_side_effects=True),
        name='pick',
    )(*users, queries[:, None])


def score_kernel(i0, i1, i2, i3, picked, final_item, scores):
    total = i0[...].astype(jnp.float32) + i1[...].astype(jnp.float32)
    total = total + i2[...].astype(jnp.float32)
    total = total + i3[...].astype(jnp.float32)
    final = (total / (LAYERS + 1)).astype(jnp.bfloat16)
    final_item[...] = final
    scores[...] = lax.dot_general(picked[...], final, NT, preferred_element_type=jnp.float32)


def score(items, picked):
    rows, emb = items[0].shape
    n_query = picked.shape[0]
    tile = 1024
    block = pl.BlockSpec((tile, emb), lambda i: (i, 0))
    return pl.pallas_call(
        score_kernel,
        grid=(rows // tile,),
        in_specs=[block] * 4 + [pl.BlockSpec((n_query, emb), lambda i: (0, 0))],
        out_specs=[block, pl.BlockSpec((n_query, tile), lambda i: (0, i))],
        out_shape=[jax.ShapeDtypeStruct((rows, emb), jnp.bfloat16),
                   jax.ShapeDtypeStruct((n_query, rows), jnp.float32)],
        compiler_params=pltpu.CompilerParams(dimension_semantics=('arbitrary',), vmem_limit_bytes=VMEM_CAP),
        name='score',
    )(*items, picked)


def solution(mesh):
    n_col = mesh.shape['col']

    def device_step(mask_blk, user_shard, item_shard, queries):
        bits, rs, cs = pack(mask_blk)
        du, di = degrees(rs, cs, n_col)
        adj = adjacency(bits, du, di)
        users, items = [user_shard], [item_shard]
        for _ in range(LAYERS):
            item_next, user_next = layer(adj, items[-1], users[-1], n_col)
            users.append(user_next)
            items.append(item_next)
        final_user, picked = pick(users, queries, n_col)
        final_item, scores = score(items, picked)
        return final_user, final_item, scores

    return jax.shard_map(device_step, mesh=mesh, in_specs=(P('row', 'col'), P(('row', 'col'), None), P(('col', 'row'), None), P()), out_specs=(P(('row', 'col'), None), P(('col', 'row'), None), P(None, ('col', 'row'))), check_vma=False)
```

```python
import functools

import jax
import jax.numpy as jnp
from jax import lax
from jax.experimental import pallas as pl
from jax.experimental.pallas import tpu as pltpu
from jax.sharding import PartitionSpec as P

LAYERS = 3
KT = 512
GROUP = 4
ROWS = 1024
RING = 4
VMEM_CAP = 67043328
MESH = pl.DeviceIdType.MESH
NT = (((1,), (1,)), ((), ()))


def pack_kernel(mask, bits, rs_ref, cs_ref, buf, out, row_acc, in_sem, out_sem):
    rows, cols = mask.shape
    steps = cols // KT

    def columns(i):
        return pl.ds(pl.multiple_of(i * KT, KT), KT)

    def load(i):
        slot = lax.rem(i, RING)
        return pltpu.make_async_copy(mask.at[:, columns(i)], buf.at[slot], in_sem.at[slot])

    def save(i):
        slot = lax.rem(i, 2)
        return pltpu.make_async_copy(out.at[slot], bits.at[:, columns(i)], out_sem.at[slot])

    for i in range(RING - 1):
        load(i).start()
    row_acc[...] = jnp.zeros_like(row_acc)

    def step(i, carry):
        slot = lax.rem(i, RING)

        @pl.when(i + RING - 1 < steps)
        def _():
            load(i + RING - 1).start()

        @pl.when(i >= 2)
        def _():
            save(i - 2).wait()

        load(i).wait()

        def block(b, col_acc):
            words = []
            for k in range(2):
                word = jnp.zeros((8, KT), jnp.int32)
                for j in range(16):
                    at = pl.ds(pl.multiple_of(b * 256 + j * 16 + k * 8, 8), 8)
                    m = buf[slot, at, :]
                    word = word | (lax.shift_left(m, j) if j else m)
                    col_acc = col_acc + m
                    part = m[:, :128]
                    for t in range(1, KT // 128):
                        part = part + m[:, t * 128:(t + 1) * 128]
                    row_acc[at, :] += part
                words.append(word)
            out[lax.rem(i, 2), pl.ds(pl.multiple_of(b * 16, 16), 16), :] = jnp.concatenate(words, axis=0).astype(jnp.int16)
            return col_acc

        col_acc = lax.fori_loop(0, rows // 256, block, jnp.zeros((8, KT), jnp.int32))
        cs_ref[:, columns(i)] = jnp.sum(col_acc, axis=0, keepdims=True)
        save(i).start()
        return carry

    lax.fori_loop(0, steps, step, 0)
    for g in range(rows // 128):
        rs_ref[g:g + 1, :] = jnp.sum(row_acc[g * 128:(g + 1) * 128, :].T, axis=0, keepdims=True)
    save(steps - 2).wait()
    save(steps - 1).wait()


def pack(mask_blk):
    rows, cols = mask_blk.shape
    vmem = pl.BlockSpec(memory_space=pltpu.VMEM)
    anyspace = pl.BlockSpec(memory_space=pl.ANY)
    return pl.pallas_call(
        pack_kernel,
        in_specs=[anyspace],
        out_specs=[anyspace, vmem, vmem],
        out_shape=[jax.ShapeDtypeStruct((rows // 16, cols), jnp.int16),
                   jax.ShapeDtypeStruct((rows // 128, 128), jnp.int32),
                   jax.ShapeDtypeStruct((1, cols), jnp.int32)],
        scratch_shapes=[pltpu.VMEM((RING, rows, KT), jnp.int32), pltpu.VMEM((2, rows // 16, KT), jnp.int16),
                        pltpu.VMEM((rows, 128), jnp.int32),
                        pltpu.SemaphoreType.DMA((RING,)), pltpu.SemaphoreType.DMA((2,))],
        compiler_params=pltpu.CompilerParams(vmem_limit_bytes=VMEM_CAP),
        name='pack',
    )(mask_blk)


def greet(peers):
    barrier = pltpu.get_barrier_semaphore()
    for dev in peers:
        pl.semaphore_signal(barrier, inc=1, device_id=dev, device_id_type=MESH)
    pl.semaphore_wait(barrier, len(peers))


def expand(bits, du, di, out):
    cols = out.shape[1]
    wide = jnp.broadcast_to(di, (16, cols))
    zero = jnp.zeros((16, cols), jnp.bfloat16)
    for b in range(out.shape[0] // 256):
        word = bits[b * 16:(b + 1) * 16, :]
        for j in range(16):
            at = b * 256 + j * 16
            value = jnp.concatenate([du[at:at + 16, :]] * (cols // 128), axis=1) * wide
            hit = (word & jnp.int16(1 << j if j < 15 else -32768)) != 0
            out[at:at + 16, :] = jnp.where(hit, value.astype(jnp.bfloat16), zero)


def spread_kernel(n_col, bits, rs_ref, cs_ref, item0, user0, query, adj, final_item, final_user, picked,
                  abuf, bwin, panel, stash, acc, upan, ut, unew, user_sum, di, rs_in, ix_in, ix_out, mine, parts,
                  deg_in, cnt_in,
                  a_sem, st_sem, b_sem, own_sem, uown_sem, f_sem, deg_send, deg_recv, cnt_send, cnt_recv,
                  p_send, p_recv, u_send, u_recv, r_send, r_recv, x_send, x_recv, one_send, one_recv, two_send, two_recv):
    col, row = lax.axis_index('col'), lax.axis_index('row')
    other = (col, 1 - row)
    n_dev = 2 * n_col
    chunks = adj.shape[0]
    half = chunks // 2
    groups = half // GROUP
    steps = 2 * groups
    rows, emb = acc.shape[1], acc.shape[2]
    wide = GROUP * KT
    own_items = half * KT
    own_rows = rows // n_col
    sides = [(lax.rem(col + o, n_col), row) for o in range(1, n_col)]
    me = col * 2 + row

    def device(o):
        lin = lax.rem(me + o, n_dev)
        return lin, (lin // 2, lin % 2)

    def remote(src, dst, send, recv, dest):
        return pltpu.make_async_remote_copy(src_ref=src, dst_ref=dst, send_sem=send, recv_sem=recv,
                                            device_id=dest, device_id_type=MESH)

    greet([device(o)[1] for o in range(1, n_dev)])

    counts = [remote(cs_ref, cnt_in, cnt_send, cnt_recv, other)]
    counts += [remote(rs_ref, deg_in.at[i], deg_send.at[i], deg_recv.at[i], sides[i]) for i in range(n_col - 1)]
    for copy in counts:
        copy.start()

    def turn(phase, pos):
        return lax.rem(phase + pos, groups)

    def item_rows(side, g):
        return pl.ds(pl.multiple_of(side * own_items + g * wide, wide), wide)

    def give_panel(g):
        return remote(panel.at[item_rows(0, g), :], panel.at[item_rows(1, g), :], p_send.at[g], p_recv.at[g], other)

    def first_panel(g):
        return remote(item0.at[item_rows(0, g), :], panel.at[item_rows(1, g), :], p_send.at[g], p_recv.at[g], other)

    def own_panel(side):
        return pltpu.make_async_copy(item0, panel.at[pl.ds(side * own_items, own_items), :], own_sem)

    def chunk_of(near, g):
        return jnp.where(near, row, 1 - row) * half + g * GROUP

    def bits_copy(u, slot):
        at = chunk_of(u < groups, lax.rem(u, groups)) * KT
        return pltpu.make_async_copy(bits.at[:, pl.ds(pl.multiple_of(at, wide), wide)], bwin.at[slot], b_sem.at[slot])

    def adj_group(chunk):
        return adj.at[pl.ds(chunk, GROUP)]

    def ring_group(slot):
        return abuf.at[pl.ds(slot * GROUP, GROUP)]

    bits_copy(0, 0).start()
    bits_copy(1, 1).start()
    own_panel(0).start()
    for g in range(groups):
        first_panel(g).start()

    def user_sends(src):
        return [remote(src, upan.at[col], u_send.at[i], u_recv.at[i], sides[i]) for i in range(n_col - 1)]

    for copy in user_sends(user0):
        copy.start()
    upan[col] = user0[...]
    user_sum[...] = user0[...].astype(jnp.float32)
    acc[0] = jnp.zeros(acc.shape[1:], acc.dtype)

    for copy in counts:
        copy.wait()
    degree = rs_ref[...]
    for i in range(n_col - 1):
        degree = degree + deg_in[i]
    inv_user = lax.rsqrt(jnp.maximum(degree, 1).astype(jnp.float32))
    du = acc.at[1, :, pl.ds(0, 128)]
    for g in range(rows // 128):
        du[g * 128:(g + 1) * 128, :] = jnp.broadcast_to(inv_user[g:g + 1, :], (128, 128)).T
    di[...] = lax.rsqrt(jnp.maximum(cs_ref[...] + cnt_in[...], 1).astype(jnp.float32))

    def make_group(u, slot, base):
        at = chunk_of(u < groups, lax.rem(u, groups)) * KT
        for k in range(GROUP):
            scale = di[:, pl.ds(pl.multiple_of(at + k * KT, KT), KT)]
            expand(bwin.at[slot, :, pl.ds(k * KT, KT)], du, scale, abuf.at[base + k])

    def user_product(layer, base, where):
        table = panel[where, :]
        for m in range(0, rows, ROWS):
            m_rows = pl.ds(m, ROWS)
            left = jnp.concatenate([abuf[base + k, m_rows, :] for k in range(GROUP)], axis=1)
            acc[layer % 2, m_rows, :] += jnp.dot(left, table, preferred_element_type=jnp.float32)

    def save(u, slot):
        return pltpu.make_async_copy(ring_group(slot), adj_group(chunk_of(u < groups, lax.rem(u, groups))), st_sem.at[slot])

    def fetch(chunk, slot):
        return pltpu.make_async_copy(adj_group(chunk), ring_group(slot), a_sem.at[slot])

    bits_copy(0, 0).wait()
    make_group(0, 0, 0)
    save(0, 0).start()
    own_panel(0).wait()
    last = groups - 1

    def first_step(i, carry):
        @pl.when(i > 0)
        def _():
            save(2 * i - 1, 1).wait()

        @pl.when(2 * i == groups)
        def _():
            for g in range(groups):
                first_panel(g).wait()

        @pl.when(i == last)
        def _():
            fetch(chunk_of(False, groups - 3), 2).start()

        again = jnp.where(i < last, 2 * i + 2, 2 * i)
        bits_copy(again, 0).start()
        bits_copy(2 * i + 1, 1).wait()
        make_group(2 * i + 1, 1, GROUP)
        user_product(0, 0, pl.ds(pl.multiple_of(2 * i * wide, wide), wide))
        save(2 * i + 1, 1).start()
        save(2 * i, 0).wait()

        @pl.when(i < last)
        def _():
            bits_copy(2 * i + 3, 1).start()

        bits_copy(again, 0).wait()
        make_group(again, 0, 0)
        user_product(0, GROUP, pl.ds(pl.multiple_of((2 * i + 1) * wide, wide), wide))

        @pl.when(i < last)
        def _():
            save(2 * i + 2, 0).start()

        return carry

    lax.fori_loop(0, groups, first_step, 0)
    save(steps - 1, 1).wait()

    def ring_slot(phase, pos):
        return lax.rem(5 * phase + pos, 3)

    def phase_chunk(phase, pos):
        users_first = phase % 2 == 0
        near = pos < groups if users_first else pos >= groups
        return chunk_of(near, turn(phase, pos))

    def stream(phase, pos):
        @pl.when((pos >= 1) & (pos + 2 < steps))
        def _():
            fetch(phase_chunk(phase, pos + 2), ring_slot(phase, pos + 2)).start()

        if phase == 1:
            @pl.when(pos == 0)
            def _():
                fetch(phase_chunk(phase, 0), ring_slot(phase, 0)).wait()

        @pl.when(pos >= 3)
        def _():
            fetch(phase_chunk(phase, pos), ring_slot(phase, pos)).wait()

        return ring_slot(phase, pos) * GROUP

    def shares(layer):
        out = []
        for i in range(n_col - 1):
            at = pl.multiple_of(sides[i][0] * own_rows, own_rows)
            out.append(remote(acc.at[layer % 2, pl.ds(at, own_rows), :], rs_in.at[i], r_send.at[i], r_recv.at[i], sides[i]))
        return out

    def user_rows(layer):
        for copy in shares(layer):
            copy.wait()
        total = acc[layer % 2, pl.ds(pl.multiple_of(col * own_rows, own_rows), own_rows), :]
        for i in range(n_col - 1):
            total = total + rs_in[i]
        fresh = total.astype(jnp.bfloat16)
        user_sum[...] += fresh.astype(jnp.float32)
        return fresh

    def user_phase(layer):
        phase = 2 * layer
        acc[layer % 2] = jnp.zeros(acc.shape[1:], acc.dtype)

        def step(pos, carry):
            base = stream(phase, pos)

            @pl.when(pos == 2)
            def _():
                unew[...] = user_rows(layer - 1)
                upan[col] = unew[...]
                for copy in user_sends(unew):
                    copy.start()

            @pl.when(pos == groups)
            def _():
                for g in range(groups):
                    give_panel(g).wait()

            where = item_rows(jnp.where(pos < groups, 0, 1), turn(phase, pos))
            user_product(layer, base, where)
            return carry

        lax.fori_loop(0, steps, step, 0)

    def give_copy(phase, q, k):
        slot = lax.rem(q, 2) * GROUP + k
        j = turn(phase, q) * GROUP + k
        return remote(ix_out.at[slot], ix_in.at[j], x_send.at[slot], x_recv.at[j], other)

    def item_phase(layer):
        phase = 2 * layer + 1
        final = layer == LAYERS - 1
        for copy in user_sends(user0 if layer == 0 else unew):
            copy.wait()
        for c in range(n_col):
            ut[:, c * own_rows:(c + 1) * own_rows] = upan[c].T
        for copy in shares(layer):
            copy.start()
        if final:
            own_panel(1).start()

        def give_step(pos, carry):
            base = stream(phase, pos)

            @pl.when(pos >= 2)
            def _():
                for k in range(GROUP):
                    give_copy(phase, pos - 2, k).wait_send()

            for k in range(GROUP):
                ix_out[lax.rem(pos, 2) * GROUP + k] = jnp.dot(ut[...], abuf[base + k], preferred_element_type=jnp.float32)
                give_copy(phase, pos, k).start()
            return carry

        lax.fori_loop(0, groups, give_step, 0)
        if final:
            own_panel(1).wait()

        def keep_step(pos, carry):
            base = stream(phase, pos)
            q = pos - groups
            g = turn(phase, pos)
            for k in range(GROUP):
                give_copy(phase, q, k).wait_recv()
            for k in range(GROUP):
                part = jnp.dot(ut[...], abuf[base + k], preferred_element_type=jnp.float32)
                fresh = (part + ix_in[g * GROUP + k]).astype(jnp.bfloat16).T
                at = pl.multiple_of(g * wide + k * KT, KT)
                here = pl.ds(at, KT)
                if layer == 0:
                    stash[here, :] = fresh
                if final:
                    total = panel[pl.ds(own_items + at, KT), :].astype(jnp.float32) + stash[here, :].astype(jnp.float32)
                    total = total + panel[here, :].astype(jnp.float32)
                    total = total + fresh.astype(jnp.float32)
                    fresh = (total / (LAYERS + 1)).astype(jnp.bfloat16)
                panel[here, :] = fresh
            if final:
                pltpu.make_async_copy(panel.at[item_rows(0, g), :], final_item.at[item_rows(0, g), :], f_sem.at[g]).start()
            else:
                give_panel(g).start()
            return carry

        lax.fori_loop(groups, steps, keep_step, 0)
        for q in range(groups - 2, groups):
            for k in range(GROUP):
                give_copy(phase, q, k).wait_send()

    item_phase(0)
    for layer in range(1, LAYERS):
        user_phase(layer)
        item_phase(layer)

    user_rows(LAYERS - 1)
    final = (user_sum[...] / (LAYERS + 1)).astype(jnp.bfloat16)
    final_user[...] = final
    share = picked.shape[0] // n_dev
    local = query[...] - (row * n_col + col) * own_rows
    hot = lax.broadcasted_iota(jnp.int32, (query.shape[0], own_rows), 1) == local
    mine[...] = jnp.dot(hot.astype(jnp.bfloat16), final, preferred_element_type=jnp.float32).astype(jnp.bfloat16)

    def rows_of(lin):
        return pl.ds(pl.multiple_of(lin * share, share), share)

    first = []
    for o in range(1, n_dev):
        lin, dest = device(o)
        first.append(remote(mine.at[rows_of(lin), :], parts.at[o - 1], one_send.at[o - 1], one_recv.at[o - 1], dest))
    for copy in first:
        copy.start()
    for copy in first:
        copy.wait()
    found = mine[rows_of(me), :].astype(jnp.float32)
    for o in range(1, n_dev):
        found = found + parts[o - 1].astype(jnp.float32)
    picked[rows_of(me), :] = found.astype(jnp.bfloat16)
    second = []
    for o in range(1, n_dev):
        here = picked.at[rows_of(me), :]
        second.append(remote(here, here, two_send.at[o - 1], two_recv.at[o - 1], device(o)[1]))
    for copy in second:
        copy.start()
    for copy in second:
        copy.wait()
    for g in range(groups):
        pltpu.make_async_copy(panel.at[item_rows(0, g), :], final_item.at[item_rows(0, g), :], f_sem.at[g]).wait()


def spread(bits, rs, cs, item_own, user_own, queries, n_col):
    items, emb = item_own.shape
    users = user_own.shape[0]
    rows, cols = n_col * users, cs.shape[1]
    chunks = cols // KT
    half = chunks // 2
    groups = half // GROUP
    n_dev = 2 * n_col
    n_query = queries.shape[0]
    anyspace = pl.BlockSpec(memory_space=pl.ANY)
    vmem = pl.BlockSpec(memory_space=pltpu.VMEM)
    dma = pltpu.SemaphoreType.DMA
    side = dma((n_col - 1,))
    all_dev = dma((n_dev - 1,))
    bf16, f32 = jnp.bfloat16, jnp.float32
    return pl.pallas_call(
        functools.partial(spread_kernel, n_col),
        in_specs=[anyspace, vmem, vmem, anyspace, vmem, vmem],
        out_specs=[anyspace, anyspace, vmem, vmem],
        out_shape=[jax.ShapeDtypeStruct((chunks, rows, KT), bf16),
                   jax.ShapeDtypeStruct((items, emb), bf16),
                   jax.ShapeDtypeStruct((users, emb), bf16),
                   jax.ShapeDtypeStruct((n_query, emb), bf16)],
        scratch_shapes=[
            pltpu.VMEM((3 * GROUP, rows, KT), bf16),
            pltpu.VMEM((2, rows // 16, GROUP * KT), jnp.int16),
            pltpu.VMEM((2 * items, emb), bf16),
            pltpu.VMEM((items, emb), bf16),
            pltpu.VMEM((2, rows, emb), f32),
            pltpu.VMEM((n_col, users, emb), bf16),
            pltpu.VMEM((emb, rows), bf16),
            pltpu.VMEM((users, emb), bf16),
            pltpu.VMEM((users, emb), f32),
            pltpu.VMEM((1, cols), f32),
            pltpu.VMEM((n_col - 1, users, emb), f32),
            pltpu.VMEM((half, emb, KT), f32),
            pltpu.VMEM((2 * GROUP, emb, KT), f32),
            pltpu.VMEM((n_query, emb), bf16),
            pltpu.VMEM((n_dev - 1, n_query // n_dev, emb), bf16),
            pltpu.VMEM((n_col - 1,) + rs.shape, jnp.int32),
            pltpu.VMEM(cs.shape, jnp.int32),
            dma((3,)), dma((2,)), dma((2,)), dma, dma, dma((groups,)), side, side, dma, dma,
            dma((groups,)), dma((groups,)), side, side, side, side, dma((2 * GROUP,)), dma((half,)),
            all_dev, all_dev, all_dev, all_dev,
        ],
        cost_estimate=pl.CostEstimate(flops=4 * LAYERS * rows * cols * emb, bytes_accessed=rows * cols * 10, transcendentals=0),
        compiler_params=pltpu.CompilerParams(collective_id=0, has_side_effects=True, vmem_limit_bytes=VMEM_CAP),
        name='spread',
    )(bits, rs, cs, item_own, user_own, queries[:, None])


def score_kernel(item, picked, final_item, scores):
    final_item[...] = item[...]
    scores[...] = lax.dot_general(picked[...], item[...], NT, preferred_element_type=jnp.float32)


def score(items, picked):
    rows, emb = items.shape
    n_query = picked.shape[0]
    tile = 1024 if rows % 1024 == 0 else rows
    block = pl.BlockSpec((tile, emb), lambda i: (i, 0))
    return pl.pallas_call(
        score_kernel,
        grid=(rows // tile,),
        in_specs=[block, pl.BlockSpec((n_query, emb), lambda i: (0, 0))],
        out_specs=[block, pl.BlockSpec((n_query, tile), lambda i: (0, i))],
        out_shape=[jax.ShapeDtypeStruct((rows, emb), jnp.bfloat16),
                   jax.ShapeDtypeStruct((n_query, rows), jnp.float32)],
        compiler_params=pltpu.CompilerParams(dimension_semantics=('arbitrary',), vmem_limit_bytes=VMEM_CAP),
        name='score',
    )(items, picked)


def solution(mesh):
    n_col = mesh.shape['col']

    def device_step(mask_blk, user_shard, item_shard, queries):
        bits, rs, cs = pack(mask_blk)
        _, item_sum, final_user, picked = spread(bits, rs, cs, item_shard, user_shard, queries, n_col)
        final_item, scores = score(item_sum, picked)
        return final_user, final_item, scores

    return jax.shard_map(device_step, mesh=mesh, in_specs=(P('row', 'col'), P(('row', 'col'), None), P(('col', 'row'), None), P()), out_specs=(P(('row', 'col'), None), P(('col', 'row'), None), P(None, ('col', 'row'))), check_vma=False)
```

```python
import functools

import jax
import jax.numpy as jnp
from jax import lax
from jax.experimental import pallas as pl
from jax.experimental.pallas import tpu as pltpu
from jax.sharding import PartitionSpec as P

LAYERS = 3
KT = 512
GROUP = 4
RING = 4
VMEM_CAP = 67043328
MESH = pl.DeviceIdType.MESH
NT = (((1,), (1,)), ((), ()))
TN = (((0,), (0,)), ((), ()))


def pack_kernel(mask, bits, rs_ref, cs_ref, buf, out, row_acc, in_sem, out_sem):
    rows, cols = mask.shape
    steps = cols // KT

    def columns(i):
        return pl.ds(pl.multiple_of(i * KT, KT), KT)

    def load(i):
        slot = lax.rem(i, RING)
        return pltpu.make_async_copy(mask.at[:, columns(i)], buf.at[slot], in_sem.at[slot])

    def save(i):
        slot = lax.rem(i, 2)
        return pltpu.make_async_copy(out.at[slot], bits.at[i], out_sem.at[slot])

    for i in range(RING - 1):
        load(i).start()
    row_acc[...] = jnp.zeros_like(row_acc)

    def step(i, carry):
        slot = lax.rem(i, RING)

        @pl.when(i + RING - 1 < steps)
        def _():
            load(i + RING - 1).start()

        @pl.when(i >= 2)
        def _():
            save(i - 2).wait()

        load(i).wait()

        def block(b, col_acc):
            words = []
            for k in range(2):
                word = jnp.zeros((8, KT), jnp.int32)
                for j in range(16):
                    at = pl.ds(pl.multiple_of(b * 256 + j * 16 + k * 8, 8), 8)
                    m = buf[slot, at, :]
                    word = word | (lax.shift_left(m, j) if j else m)
                    col_acc = col_acc + m
                    part = m[:, :128]
                    for t in range(1, KT // 128):
                        part = part + m[:, t * 128:(t + 1) * 128]
                    row_acc[at, :] += part
                words.append(word)
            out[lax.rem(i, 2), pl.ds(pl.multiple_of(b * 16, 16), 16), :] = jnp.concatenate(words, axis=0).astype(jnp.int16)
            return col_acc

        col_acc = lax.fori_loop(0, rows // 256, block, jnp.zeros((8, KT), jnp.int32))
        cs_ref[:, columns(i)] = jnp.sum(col_acc, axis=0, keepdims=True)
        save(i).start()
        return carry

    lax.fori_loop(0, steps, step, 0)
    for g in range(rows // 128):
        rs_ref[g:g + 1, :] = jnp.sum(row_acc[g * 128:(g + 1) * 128, :].T, axis=0, keepdims=True)
    save(steps - 2).wait()
    save(steps - 1).wait()


def pack(mask_blk):
    rows, cols = mask_blk.shape
    steps = cols // KT
    vmem = pl.BlockSpec(memory_space=pltpu.VMEM)
    anyspace = pl.BlockSpec(memory_space=pl.ANY)
    return pl.pallas_call(
        pack_kernel,
        in_specs=[anyspace],
        out_specs=[anyspace, vmem, vmem],
        out_shape=[jax.ShapeDtypeStruct((steps, rows // 16, KT), jnp.int16),
                   jax.ShapeDtypeStruct((rows // 128, 128), jnp.int32),
                   jax.ShapeDtypeStruct((1, cols), jnp.int32)],
        scratch_shapes=[pltpu.VMEM((RING, rows, KT), jnp.int32), pltpu.VMEM((2, rows // 16, KT), jnp.int16),
                        pltpu.VMEM((rows, 128), jnp.int32),
                        pltpu.SemaphoreType.DMA((RING,)), pltpu.SemaphoreType.DMA((2,))],
        compiler_params=pltpu.CompilerParams(vmem_limit_bytes=VMEM_CAP),
        name='pack',
    )(mask_blk)


def greet(peers):
    barrier = pltpu.get_barrier_semaphore()
    for dev in peers:
        pl.semaphore_signal(barrier, inc=1, device_id=dev, device_id_type=MESH)
    pl.semaphore_wait(barrier, len(peers))


def expand(bits, du, di, place, b):
    lanes = di.shape[1] // 128
    wide = jnp.concatenate([du[b * 256:(b + 1) * 256, :]] * lanes, axis=1)
    word = jnp.concatenate([bits[b * 16:(b + 1) * 16, :]] * 16, axis=0)
    hit = (word & jnp.concatenate([place[...]] * lanes, axis=1)) != 0
    value = (wide * di).astype(jnp.bfloat16)
    return jnp.where(hit, value, jnp.zeros_like(value))


def spread_kernel(n_col, bits, rs_ref, cs_ref, item0, user0, query, final_item, final_user, picked,
                  words, du, place, panel, stash, acc, upan, ut, unew, user_sum, di, rs_in, ix_in, ix_out, mine, parts,
                  deg_in, cnt_in,
                  b_sem, own_sem, f_sem, deg_send, deg_recv, cnt_send, cnt_recv,
                  p_send, p_recv, u_send, u_recv, r_send, r_recv, x_send, x_recv, one_send, one_recv, two_send, two_recv):
    col, row = lax.axis_index('col'), lax.axis_index('row')
    other = (col, 1 - row)
    n_dev = 2 * n_col
    chunks = bits.shape[0]
    half = chunks // 2
    groups = half // GROUP
    steps = 2 * groups
    rows, emb = acc.shape[1], acc.shape[2]
    wide = GROUP * KT
    own_items = half * KT
    own_rows = rows // n_col
    sides = [(lax.rem(col + o, n_col), row) for o in range(1, n_col)]
    me = col * 2 + row

    def device(o):
        lin = lax.rem(me + o, n_dev)
        return lin, (lin // 2, lin % 2)

    def remote(src, dst, send, recv, dest):
        return pltpu.make_async_remote_copy(src_ref=src, dst_ref=dst, send_sem=send, recv_sem=recv,
                                            device_id=dest, device_id_type=MESH)

    greet([device(o)[1] for o in range(1, n_dev)])

    counts = [remote(cs_ref, cnt_in, cnt_send, cnt_recv, other)]
    counts += [remote(rs_ref, deg_in.at[i], deg_send.at[i], deg_recv.at[i], sides[i]) for i in range(n_col - 1)]
    for copy in counts:
        copy.start()

    def turn(phase, pos):
        return lax.rem(phase + pos, groups)

    def item_rows(side, g):
        return pl.ds(pl.multiple_of(side * own_items + g * wide, wide), wide)

    def give_panel(g):
        return remote(panel.at[item_rows(0, g), :], panel.at[item_rows(1, g), :], p_send.at[g], p_recv.at[g], other)

    def first_panel(g):
        return remote(item0.at[item_rows(0, g), :], panel.at[item_rows(1, g), :], p_send.at[g], p_recv.at[g], other)

    def own_panel(side):
        return pltpu.make_async_copy(item0, panel.at[pl.ds(side * own_items, own_items), :], own_sem)

    def chunk_of(near, g):
        return jnp.where(near, row, 1 - row) * half + g * GROUP

    words_copy = pltpu.make_async_copy(bits, words, b_sem)
    words_copy.start()
    own_panel(0).start()
    for g in range(groups):
        first_panel(g).start()

    def user_sends(src):
        return [remote(src, upan.at[col], u_send.at[i], u_recv.at[i], sides[i]) for i in range(n_col - 1)]

    for copy in user_sends(user0):
        copy.start()
    upan[col] = user0[...]
    for j in range(16):
        place[j * 16:(j + 1) * 16, :] = jnp.full((16, 128), 1 << j if j < 15 else -32768, jnp.int16)
    user_sum[...] = user0[...].astype(jnp.float32)

    for copy in counts:
        copy.wait()
    degree = rs_ref[...]
    for i in range(n_col - 1):
        degree = degree + deg_in[i]
    inv_user = lax.rsqrt(jnp.maximum(degree, 1).astype(jnp.float32))
    for g in range(rows // 128):
        du[g * 128:(g + 1) * 128, :] = jnp.broadcast_to(inv_user[g:g + 1, :], (128, 128)).T
    di[...] = lax.rsqrt(jnp.maximum(cs_ref[...] + cnt_in[...], 1).astype(jnp.float32))

    def scale_of(chunk):
        return di[:, pl.ds(pl.multiple_of(chunk * KT, KT), KT)]

    def user_product(layer, chunk, where):
        scale = [scale_of(chunk + k) for k in range(GROUP)]
        for b in range(rows // 256):
            left = jnp.concatenate([expand(words.at[chunk + k], du, scale[k], place, b) for k in range(GROUP)], axis=1)
            acc[layer % 2, b * 256:(b + 1) * 256, :] += jnp.dot(left, panel[where, :], preferred_element_type=jnp.float32)

    def item_product(chunk):
        scale = scale_of(chunk)
        right = jnp.concatenate([expand(words.at[chunk], du, scale, place, b) for b in range(rows // 256)], axis=0)
        return jnp.dot(ut[...], right, preferred_element_type=jnp.float32)

    def phase_chunk(phase, pos):
        users_first = phase % 2 == 0
        near = (pos < groups) == users_first
        return chunk_of(near, turn(phase, pos))

    def shares(layer):
        out = []
        for i in range(n_col - 1):
            at = pl.multiple_of(sides[i][0] * own_rows, own_rows)
            out.append(remote(acc.at[layer % 2, pl.ds(at, own_rows), :], rs_in.at[i], r_send.at[i], r_recv.at[i], sides[i]))
        return out

    def user_rows(layer):
        for copy in shares(layer):
            copy.wait()
        total = acc[layer % 2, pl.ds(pl.multiple_of(col * own_rows, own_rows), own_rows), :]
        for i in range(n_col - 1):
            total = total + rs_in[i]
        fresh = total.astype(jnp.bfloat16)
        user_sum[...] += fresh.astype(jnp.float32)
        return fresh

    def user_phase(layer):
        phase = 2 * layer
        acc[layer % 2] = jnp.zeros(acc.shape[1:], acc.dtype)

        def step(pos, carry):
            def next_users():
                unew[...] = user_rows(layer - 1)
                upan[col] = unew[...]
                for copy in user_sends(unew):
                    copy.start()

            if layer > 0:
                pl.when(pos == 2)(next_users)

            @pl.when(pos == groups)
            def _():
                for g in range(groups):
                    (give_panel if layer > 0 else first_panel)(g).wait()

            where = item_rows(jnp.where(pos < groups, 0, 1), turn(phase, pos))
            user_product(layer, phase_chunk(phase, pos), where)
            return carry

        lax.fori_loop(0, steps, step, 0)

    def part_slot(pos):
        return lax.rem(pos, 3) * GROUP

    def give_copy(phase, q, k):
        slot = part_slot(q) + k
        j = turn(phase, q) * GROUP + k
        return remote(ix_out.at[slot], ix_in.at[j], x_send.at[slot], x_recv.at[j], other)

    def item_phase(layer):
        phase = 2 * layer + 1
        final = layer == LAYERS - 1
        for copy in user_sends(user0 if layer == 0 else unew):
            copy.wait()
        for c in range(n_col):
            ut[:, c * own_rows:(c + 1) * own_rows] = upan[c].T
        for copy in shares(layer):
            copy.start()
        if final:
            own_panel(1).start()

        def product(pos, base, k):
            ix_out[part_slot(pos) + k] = item_product(base + k)

        def sent(pos):
            for k in range(GROUP):
                give_copy(phase, pos - 3, k).wait_send()

        def give_step(pos, carry):
            base = phase_chunk(phase, pos)
            pl.when(pos >= 3)(functools.partial(sent, pos))
            for k in range(GROUP):
                product(pos, base, k)
                give_copy(phase, pos, k).start()
            return carry

        def arrived(pos):
            for k in range(GROUP):
                give_copy(phase, pos - groups, k).wait_recv()

        def finish(pos, k):
            g = turn(phase, pos)
            fresh = (ix_out[part_slot(pos) + k] + ix_in[g * GROUP + k]).astype(jnp.bfloat16).T
            at = pl.multiple_of(g * wide + k * KT, KT)
            here = pl.ds(at, KT)
            if layer == 0:
                stash[here, :] = fresh
            if final:
                total = panel[pl.ds(own_items + at, KT), :].astype(jnp.float32) + stash[here, :].astype(jnp.float32)
                total = total + panel[here, :].astype(jnp.float32)
                total = total + fresh.astype(jnp.float32)
                fresh = (total / (LAYERS + 1)).astype(jnp.bfloat16)
            panel[here, :] = fresh

        def hand_on(pos):
            g = turn(phase, pos)
            if final:
                pltpu.make_async_copy(panel.at[item_rows(0, g), :], final_item.at[item_rows(0, g), :], f_sem.at[g]).start()
            else:
                give_panel(g).start()

        def keep_step(pos, carry):
            base = phase_chunk(phase, pos)

            @pl.when(pos < groups + 3)
            def _():
                sent(pos)

            arrived(pos - 1)
            for k in range(GROUP):
                finish(pos - 1, k)
                product(pos, base, k)
            hand_on(pos - 1)
            return carry

        lax.fori_loop(0, groups, give_step, 0)
        if final:
            own_panel(1).wait()
        base = phase_chunk(phase, groups)
        sent(groups)
        for k in range(GROUP):
            product(groups, base, k)
        lax.fori_loop(groups + 1, steps, keep_step, 0)
        arrived(steps - 1)
        for k in range(GROUP):
            finish(steps - 1, k)
        hand_on(steps - 1)

    words_copy.wait()
    own_panel(0).wait()
    for layer in range(LAYERS):
        user_phase(layer)
        item_phase(layer)

    user_rows(LAYERS - 1)
    final = (user_sum[...] / (LAYERS + 1)).astype(jnp.bfloat16)
    final_user[...] = final
    share = picked.shape[0] // n_dev
    local = query[...] - (row * n_col + col) * own_rows
    hot = lax.broadcasted_iota(jnp.int32, (own_rows, query.shape[1]), 0) == local
    mine[...] = lax.dot_general(hot.astype(jnp.bfloat16), final, TN, preferred_element_type=jnp.float32).astype(jnp.bfloat16)

    def rows_of(lin):
        return pl.ds(pl.multiple_of(lin * share, share), share)

    first = []
    for o in range(1, n_dev):
        lin, dest = device(o)
        first.append(remote(mine.at[rows_of(lin), :], parts.at[o - 1], one_send.at[o - 1], one_recv.at[o - 1], dest))
    for copy in first:
        copy.start()
    for copy in first:
        copy.wait()
    found = mine[rows_of(me), :].astype(jnp.float32)
    for o in range(1, n_dev):
        found = found + parts[o - 1].astype(jnp.float32)
    picked[rows_of(me), :] = found.astype(jnp.bfloat16)
    second = []
    for o in range(1, n_dev):
        here = picked.at[rows_of(me), :]
        second.append(remote(here, here, two_send.at[o - 1], two_recv.at[o - 1], device(o)[1]))
    for copy in second:
        copy.start()
    for copy in second:
        copy.wait()
    for g in range(groups):
        pltpu.make_async_copy(panel.at[item_rows(0, g), :], final_item.at[item_rows(0, g), :], f_sem.at[g]).wait()


def spread(bits, rs, cs, item_own, user_own, queries, n_col):
    items, emb = item_own.shape
    users = user_own.shape[0]
    rows, cols = n_col * users, cs.shape[1]
    chunks = cols // KT
    half = chunks // 2
    groups = half // GROUP
    n_dev = 2 * n_col
    n_query = queries.shape[0]
    anyspace = pl.BlockSpec(memory_space=pl.ANY)
    vmem = pl.BlockSpec(memory_space=pltpu.VMEM)
    dma = pltpu.SemaphoreType.DMA
    side = dma((n_col - 1,))
    all_dev = dma((n_dev - 1,))
    bf16, f32 = jnp.bfloat16, jnp.float32
    return pl.pallas_call(
        functools.partial(spread_kernel, n_col),
        in_specs=[anyspace, vmem, vmem, anyspace, vmem, vmem],
        out_specs=[anyspace, vmem, vmem],
        out_shape=[jax.ShapeDtypeStruct((items, emb), bf16),
                   jax.ShapeDtypeStruct((users, emb), bf16),
                   jax.ShapeDtypeStruct((n_query, emb), bf16)],
        scratch_shapes=[
            pltpu.VMEM(bits.shape, jnp.int16),
            pltpu.VMEM((rows, 128), f32),
            pltpu.VMEM((256, 128), jnp.int16),
            pltpu.VMEM((2 * items, emb), bf16),
            pltpu.VMEM((items, emb), bf16),
            pltpu.VMEM((2, rows, emb), f32),
            pltpu.VMEM((n_col, users, emb), bf16),
            pltpu.VMEM((emb, rows), bf16),
            pltpu.VMEM((users, emb), bf16),
            pltpu.VMEM((users, emb), f32),
            pltpu.VMEM((1, cols), f32),
            pltpu.VMEM((n_col - 1, users, emb), f32),
            pltpu.VMEM((half, emb, KT), f32),
            pltpu.VMEM((3 * GROUP, emb, KT), f32),
            pltpu.VMEM((n_query, emb), bf16),
            pltpu.VMEM((n_dev - 1, n_query // n_dev, emb), bf16),
            pltpu.VMEM((n_col - 1,) + rs.shape, jnp.int32),
            pltpu.VMEM(cs.shape, jnp.int32),
            dma, dma, dma((groups,)), side, side, dma, dma,
            dma((groups,)), dma((groups,)), side, side, side, side, dma((3 * GROUP,)), dma((half,)),
            all_dev, all_dev, all_dev, all_dev,
        ],
        cost_estimate=pl.CostEstimate(flops=4 * LAYERS * rows * cols * emb, bytes_accessed=rows * cols, transcendentals=0),
        compiler_params=pltpu.CompilerParams(collective_id=0, has_side_effects=True, vmem_limit_bytes=VMEM_CAP),
        name='spread',
    )(bits, rs, cs, item_own, user_own, queries[None, :])


def score_kernel(user, item, picked, final_user, final_item, scores):
    final_user[...] = user[...]
    final_item[...] = item[...]
    scores[...] = lax.dot_general(picked[...], item[...], NT, preferred_element_type=jnp.float32)


def score(users, items, picked):
    rows, emb = items.shape
    n_query = picked.shape[0]
    tile = 1024 if rows % 1024 == 0 else rows
    block = pl.BlockSpec((tile, emb), lambda i: (i, 0))
    whole = pl.BlockSpec(users.shape, lambda i: (0, 0))
    return pl.pallas_call(
        score_kernel,
        grid=(rows // tile,),
        in_specs=[whole, block, pl.BlockSpec((n_query, emb), lambda i: (0, 0))],
        out_specs=[whole, block, pl.BlockSpec((n_query, tile), lambda i: (0, i))],
        out_shape=[jax.ShapeDtypeStruct(users.shape, jnp.bfloat16),
                   jax.ShapeDtypeStruct((rows, emb), jnp.bfloat16),
                   jax.ShapeDtypeStruct((n_query, rows), jnp.float32)],
        compiler_params=pltpu.CompilerParams(dimension_semantics=('arbitrary',), vmem_limit_bytes=VMEM_CAP),
        name='score',
    )(users, items, picked)


def solution(mesh):
    n_col = mesh.shape['col']

    def device_step(mask_blk, user_shard, item_shard, queries):
        bits, rs, cs = pack(mask_blk)
        item_mean, user_mean, picked = spread(bits, rs, cs, item_shard, user_shard, queries, n_col)
        final_user, final_item, scores = score(user_mean, item_mean, picked)
        return final_user, final_item, scores

    return jax.shard_map(device_step, mesh=mesh, in_specs=(P('row', 'col'), P(('row', 'col'), None), P(('col', 'row'), None), P()), out_specs=(P(('row', 'col'), None), P(('col', 'row'), None), P(None, ('col', 'row'))), check_vma=False)
```

```python
import functools

import jax
import jax.numpy as jnp
from jax import lax
from jax.experimental import pallas as pl
from jax.experimental.pallas import tpu as pltpu
from jax.sharding import PartitionSpec as P

LAYERS = 3
KT = 512
GROUP = 4
RING = 3
VMEM_CAP = 67043328
MESH = pl.DeviceIdType.MESH
NT = (((1,), (1,)), ((), ()))
TN = (((0,), (0,)), ((), ()))


def pack(mask, words, rs_ref, cs_ref, buf, row_acc, load):
    rows, cols = mask.shape
    steps = cols // KT
    row_acc[...] = jnp.zeros_like(row_acc)
    shift_of = lax.broadcasted_iota(jnp.int32, (256, KT), 0) // 16

    def step(i, carry):
        slot = lax.rem(i, RING)

        @pl.when(i + RING - 1 < steps)
        def _():
            load(i + RING - 1).start()

        load(i).wait()

        def block(b, col_acc):
            at = pl.ds(pl.multiple_of(b * 256, 256), 256)
            m = buf[slot, at, :]
            part = m[:, :128]
            for t in range(1, KT // 128):
                part = part + m[:, t * 128:(t + 1) * 128]
            row_acc[at, :] += part
            weighed = (m << shift_of).reshape(16, 16, KT)
            words[i, pl.ds(pl.multiple_of(b * 16, 16), 16), :] = jnp.sum(weighed, axis=0).astype(jnp.int16)
            return col_acc + jnp.sum(m.reshape(32, 8, KT), axis=0)

        col_acc = lax.fori_loop(0, rows // 256, block, jnp.zeros((8, KT), jnp.int32))
        cs_ref[:, pl.ds(pl.multiple_of(i * KT, KT), KT)] = jnp.sum(col_acc, axis=0, keepdims=True)
        return carry

    lax.fori_loop(0, steps, step, 0)
    for g in range(rows // 128):
        rs_ref[g:g + 1, :] = jnp.sum(row_acc[g * 128:(g + 1) * 128, :].T, axis=0, keepdims=True)


def greet(peers):
    barrier = pltpu.get_barrier_semaphore()
    for dev in peers:
        pl.semaphore_signal(barrier, inc=1, device_id=dev, device_id_type=MESH)
    pl.semaphore_wait(barrier, len(peers))


def expand(bits, du, di, place, b):
    lanes = di.shape[1] // 128
    wide = jnp.concatenate([du[b * 256:(b + 1) * 256, :]] * lanes, axis=1)
    word = jnp.concatenate([bits[b * 16:(b + 1) * 16, :]] * 16, axis=0)
    hit = (word & jnp.concatenate([place[...]] * lanes, axis=1)) != 0
    value = (wide * di).astype(jnp.bfloat16)
    return jnp.where(hit, value, jnp.zeros_like(value))


def spread_kernel(n_col, mask, item0, user0, query, final_item, final_user, picked,
                  buf, row_acc, rs_ref, cs_ref, words, du, place, panel, stash, acc, upan, ut, unew, user_sum, di, rs_in, ix_in, ix_out, mine, parts,
                  deg_in, cnt_in,
                  m_sem, own_sem, f_sem, deg_send, deg_recv, cnt_send, cnt_recv,
                  p_send, p_recv, u_send, u_recv, r_send, r_recv, x_send, x_recv, one_send, one_recv, two_send, two_recv):
    col, row = lax.axis_index('col'), lax.axis_index('row')
    other = (col, 1 - row)
    n_dev = 2 * n_col
    chunks = mask.shape[1] // KT
    half = chunks // 2
    groups = half // GROUP
    steps = 2 * groups
    rows, emb = acc.shape[1], acc.shape[2]
    wide = GROUP * KT
    own_items = half * KT
    own_rows = rows // n_col
    sides = [(lax.rem(col + o, n_col), row) for o in range(1, n_col)]
    me = col * 2 + row

    def device(o):
        lin = lax.rem(me + o, n_dev)
        return lin, (lin // 2, lin % 2)

    def remote(src, dst, send, recv, dest):
        return pltpu.make_async_remote_copy(src_ref=src, dst_ref=dst, send_sem=send, recv_sem=recv,
                                            device_id=dest, device_id_type=MESH)

    def load(i):
        slot = lax.rem(i, RING)
        return pltpu.make_async_copy(mask.at[:, pl.ds(pl.multiple_of(i * KT, KT), KT)], buf.at[slot], m_sem.at[slot])

    for i in range(RING - 1):
        load(jnp.int32(i)).start()
    greet([device(o)[1] for o in range(1, n_dev)])

    def user_sends(src):
        return [remote(src, upan.at[col], u_send.at[i], u_recv.at[i], sides[i]) for i in range(n_col - 1)]

    for copy in user_sends(user0):
        copy.start()
    upan[col] = user0[...]
    for j in range(16):
        place[j * 16:(j + 1) * 16, :] = jnp.full((16, 128), 1 << j if j < 15 else -32768, jnp.int16)
    user_sum[...] = user0[...].astype(jnp.float32)
    pack(mask, words, rs_ref, cs_ref, buf, row_acc, load)

    counts = [remote(cs_ref, cnt_in, cnt_send, cnt_recv, other)]
    counts += [remote(rs_ref, deg_in.at[i], deg_send.at[i], deg_recv.at[i], sides[i]) for i in range(n_col - 1)]
    for copy in counts:
        copy.start()

    def turn(phase, pos):
        return lax.rem(phase + pos, groups)

    def item_rows(side, g):
        return pl.ds(pl.multiple_of(side * own_items + g * wide, wide), wide)

    def give_panel(g):
        return remote(panel.at[item_rows(0, g), :], panel.at[item_rows(1, g), :], p_send.at[g], p_recv.at[g], other)

    def first_panel(g):
        return remote(item0.at[item_rows(0, g), :], panel.at[item_rows(1, g), :], p_send.at[g], p_recv.at[g], other)

    def own_panel(side):
        return pltpu.make_async_copy(item0, panel.at[pl.ds(side * own_items, own_items), :], own_sem)

    def chunk_of(near, g):
        return jnp.where(near, row, 1 - row) * half + g * GROUP

    own_panel(0).start()
    for g in range(groups):
        first_panel(g).start()

    for copy in counts:
        copy.wait()
    degree = rs_ref[...]
    for i in range(n_col - 1):
        degree = degree + deg_in[i]
    inv_user = lax.rsqrt(jnp.maximum(degree, 1).astype(jnp.float32))
    for g in range(rows // 128):
        du[g * 128:(g + 1) * 128, :] = jnp.broadcast_to(inv_user[g:g + 1, :], (128, 128)).T
    di[...] = lax.rsqrt(jnp.maximum(cs_ref[...] + cnt_in[...], 1).astype(jnp.float32))

    def scale_of(chunk):
        return di[:, pl.ds(pl.multiple_of(chunk * KT, KT), KT)]

    def user_product(layer, chunk, where):
        scale = [scale_of(chunk + k) for k in range(GROUP)]
        for b in range(rows // 256):
            left = jnp.concatenate([expand(words.at[chunk + k], du, scale[k], place, b) for k in range(GROUP)], axis=1)
            acc[layer % 2, b * 256:(b + 1) * 256, :] += jnp.dot(left, panel[where, :], preferred_element_type=jnp.float32)

    def item_product(chunk):
        scale = scale_of(chunk)
        right = jnp.concatenate([expand(words.at[chunk], du, scale, place, b) for b in range(rows // 256)], axis=0)
        return jnp.dot(ut[...], right, preferred_element_type=jnp.float32)

    def phase_chunk(phase, pos):
        users_first = phase % 2 == 0
        near = (pos < groups) == users_first
        return chunk_of(near, turn(phase, pos))

    def shares(layer):
        out = []
        for i in range(n_col - 1):
            at = pl.multiple_of(sides[i][0] * own_rows, own_rows)
            out.append(remote(acc.at[layer % 2, pl.ds(at, own_rows), :], rs_in.at[i], r_send.at[i], r_recv.at[i], sides[i]))
        return out

    def user_rows(layer):
        for copy in shares(layer):
            copy.wait()
        total = acc[layer % 2, pl.ds(pl.multiple_of(col * own_rows, own_rows), own_rows), :]
        for i in range(n_col - 1):
            total = total + rs_in[i]
        fresh = total.astype(jnp.bfloat16)
        user_sum[...] += fresh.astype(jnp.float32)
        return fresh

    def user_phase(layer):
        phase = 2 * layer
        acc[layer % 2] = jnp.zeros(acc.shape[1:], acc.dtype)

        def step(pos, carry):
            def next_users():
                unew[...] = user_rows(layer - 1)
                upan[col] = unew[...]
                for copy in user_sends(unew):
                    copy.start()

            if layer > 0:
                pl.when(pos == 2)(next_users)

            @pl.when(pos == groups)
            def _():
                for g in range(groups):
                    (give_panel if layer > 0 else first_panel)(g).wait()

            where = item_rows(jnp.where(pos < groups, 0, 1), turn(phase, pos))
            user_product(layer, phase_chunk(phase, pos), where)
            return carry

        lax.fori_loop(0, steps, step, 0)

    def part_slot(pos):
        return lax.rem(pos, 3) * GROUP

    def give_copy(phase, q, k):
        slot = part_slot(q) + k
        j = turn(phase, q) * GROUP + k
        return remote(ix_out.at[slot], ix_in.at[j], x_send.at[slot], x_recv.at[j], other)

    def item_phase(layer):
        phase = 2 * layer + 1
        final = layer == LAYERS - 1
        for copy in user_sends(user0 if layer == 0 else unew):
            copy.wait()
        for c in range(n_col):
            ut[:, c * own_rows:(c + 1) * own_rows] = upan[c].T
        for copy in shares(layer):
            copy.start()
        if final:
            own_panel(1).start()

        def product(pos, base, k):
            ix_out[part_slot(pos) + k] = item_product(base + k)

        def sent(pos):
            for k in range(GROUP):
                give_copy(phase, pos - 3, k).wait_send()

        def give_step(pos, carry):
            base = phase_chunk(phase, pos)
            pl.when(pos >= 3)(functools.partial(sent, pos))
            for k in range(GROUP):
                product(pos, base, k)
                give_copy(phase, pos, k).start()
            return carry

        def arrived(pos):
            for k in range(GROUP):
                give_copy(phase, pos - groups, k).wait_recv()

        def finish(pos, k):
            g = turn(phase, pos)
            fresh = (ix_out[part_slot(pos) + k] + ix_in[g * GROUP + k]).astype(jnp.bfloat16).T
            at = pl.multiple_of(g * wide + k * KT, KT)
            here = pl.ds(at, KT)
            if layer == 0:
                stash[here, :] = fresh
            if final:
                total = panel[pl.ds(own_items + at, KT), :].astype(jnp.float32) + stash[here, :].astype(jnp.float32)
                total = total + panel[here, :].astype(jnp.float32)
                total = total + fresh.astype(jnp.float32)
                fresh = (total / (LAYERS + 1)).astype(jnp.bfloat16)
            panel[here, :] = fresh

        def hand_on(pos):
            g = turn(phase, pos)
            if final:
                pltpu.make_async_copy(panel.at[item_rows(0, g), :], final_item.at[item_rows(0, g), :], f_sem.at[g]).start()
            else:
                give_panel(g).start()

        def keep_step(pos, carry):
            base = phase_chunk(phase, pos)

            @pl.when(pos < groups + 3)
            def _():
                sent(pos)

            arrived(pos - 1)
            for k in range(GROUP):
                finish(pos - 1, k)
                product(pos, base, k)
            hand_on(pos - 1)
            return carry

        lax.fori_loop(0, groups, give_step, 0)
        if final:
            own_panel(1).wait()
        base = phase_chunk(phase, groups)
        sent(groups)
        for k in range(GROUP):
            product(groups, base, k)
        lax.fori_loop(groups + 1, steps, keep_step, 0)
        arrived(steps - 1)
        for k in range(GROUP):
            finish(steps - 1, k)
        hand_on(steps - 1)

    own_panel(0).wait()
    for layer in range(LAYERS):
        user_phase(layer)
        item_phase(layer)

    user_rows(LAYERS - 1)
    final = (user_sum[...] / (LAYERS + 1)).astype(jnp.bfloat16)
    final_user[...] = final
    share = picked.shape[0] // n_dev
    local = query[...] - (row * n_col + col) * own_rows
    hot = lax.broadcasted_iota(jnp.int32, (own_rows, query.shape[1]), 0) == local
    mine[...] = lax.dot_general(hot.astype(jnp.bfloat16), final, TN, preferred_element_type=jnp.float32).astype(jnp.bfloat16)

    def rows_of(lin):
        return pl.ds(pl.multiple_of(lin * share, share), share)

    first = []
    for o in range(1, n_dev):
        lin, dest = device(o)
        first.append(remote(mine.at[rows_of(lin), :], parts.at[o - 1], one_send.at[o - 1], one_recv.at[o - 1], dest))
    for copy in first:
        copy.start()
    for copy in first:
        copy.wait()
    found = mine[rows_of(me), :].astype(jnp.float32)
    for o in range(1, n_dev):
        found = found + parts[o - 1].astype(jnp.float32)
    picked[rows_of(me), :] = found.astype(jnp.bfloat16)
    second = []
    for o in range(1, n_dev):
        here = picked.at[rows_of(me), :]
        second.append(remote(here, here, two_send.at[o - 1], two_recv.at[o - 1], device(o)[1]))
    for copy in second:
        copy.start()
    for copy in second:
        copy.wait()
    for g in range(groups):
        pltpu.make_async_copy(panel.at[item_rows(0, g), :], final_item.at[item_rows(0, g), :], f_sem.at[g]).wait()


def spread(mask_blk, item_own, user_own, queries, n_col):
    items, emb = item_own.shape
    users = user_own.shape[0]
    rows, cols = mask_blk.shape
    chunks = cols // KT
    half = chunks // 2
    groups = half // GROUP
    n_dev = 2 * n_col
    n_query = queries.shape[0]
    anyspace = pl.BlockSpec(memory_space=pl.ANY)
    vmem = pl.BlockSpec(memory_space=pltpu.VMEM)
    dma = pltpu.SemaphoreType.DMA
    side = dma((n_col - 1,))
    all_dev = dma((n_dev - 1,))
    bf16, f32 = jnp.bfloat16, jnp.float32
    return pl.pallas_call(
        functools.partial(spread_kernel, n_col),
        in_specs=[anyspace, anyspace, vmem, vmem],
        out_specs=[anyspace, vmem, vmem],
        out_shape=[jax.ShapeDtypeStruct((items, emb), bf16),
                   jax.ShapeDtypeStruct((users, emb), bf16),
                   jax.ShapeDtypeStruct((n_query, emb), bf16)],
        scratch_shapes=[
            pltpu.VMEM((RING, rows, KT), jnp.int32),
            pltpu.VMEM((rows, 128), jnp.int32),
            pltpu.VMEM((rows // 128, 128), jnp.int32),
            pltpu.VMEM((1, cols), jnp.int32),
            pltpu.VMEM((chunks, rows // 16, KT), jnp.int16),
            pltpu.VMEM((rows, 128), f32),
            pltpu.VMEM((256, 128), jnp.int16),
            pltpu.VMEM((2 * items, emb), bf16),
            pltpu.VMEM((items, emb), bf16),
            pltpu.VMEM((2, rows, emb), f32),
            pltpu.VMEM((n_col, users, emb), bf16),
            pltpu.VMEM((emb, rows), bf16),
            pltpu.VMEM((users, emb), bf16),
            pltpu.VMEM((users, emb), f32),
            pltpu.VMEM((1, cols), f32),
            pltpu.VMEM((n_col - 1, users, emb), f32),
            pltpu.VMEM((half, emb, KT), f32),
            pltpu.VMEM((3 * GROUP, emb, KT), f32),
            pltpu.VMEM((n_query, emb), bf16),
            pltpu.VMEM((n_dev - 1, n_query // n_dev, emb), bf16),
            pltpu.VMEM((n_col - 1, rows // 128, 128), jnp.int32),
            pltpu.VMEM((1, cols), jnp.int32),
            dma((RING,)), dma, dma((groups,)), side, side, dma, dma,
            dma((groups,)), dma((groups,)), side, side, side, side, dma((3 * GROUP,)), dma((half,)),
            all_dev, all_dev, all_dev, all_dev,
        ],
        cost_estimate=pl.CostEstimate(flops=4 * LAYERS * rows * cols * emb, bytes_accessed=rows * cols * 4, transcendentals=0),
        compiler_params=pltpu.CompilerParams(collective_id=0, has_side_effects=True, vmem_limit_bytes=VMEM_CAP),
        name='spread',
    )(mask_blk, item_own, user_own, queries[None, :])


def score_kernel(user, item, picked, final_user, final_item, scores):
    final_user[...] = user[...]
    final_item[...] = item[...]
    scores[...] = lax.dot_general(picked[...], item[...], NT, preferred_element_type=jnp.float32)


def score(users, items, picked):
    rows, emb = items.shape
    n_query = picked.shape[0]
    tile = 2048 if rows % 2048 == 0 else rows
    block = pl.BlockSpec((tile, emb), lambda i: (i, 0))
    whole = pl.BlockSpec(users.shape, lambda i: (0, 0))
    return pl.pallas_call(
        score_kernel,
        grid=(rows // tile,),
        in_specs=[whole, block, pl.BlockSpec((n_query, emb), lambda i: (0, 0))],
        out_specs=[whole, block, pl.BlockSpec((n_query, tile), lambda i: (0, i))],
        out_shape=[jax.ShapeDtypeStruct(users.shape, jnp.bfloat16),
                   jax.ShapeDtypeStruct((rows, emb), jnp.bfloat16),
                   jax.ShapeDtypeStruct((n_query, rows), jnp.float32)],
        compiler_params=pltpu.CompilerParams(dimension_semantics=('arbitrary',), vmem_limit_bytes=VMEM_CAP),
        name='score',
    )(users, items, picked)


def solution(mesh):
    n_col = mesh.shape['col']

    def device_step(mask_blk, user_shard, item_shard, queries):
        item_mean, user_mean, picked = spread(mask_blk, item_shard, user_shard, queries, n_col)
        final_user, final_item, scores = score(user_mean, item_mean, picked)
        return final_user, final_item, scores

    return jax.shard_map(device_step, mesh=mesh, in_specs=(P('row', 'col'), P(('row', 'col'), None), P(('col', 'row'), None), P()), out_specs=(P(('row', 'col'), None), P(('col', 'row'), None), P(None, ('col', 'row'))), check_vma=False)
```
